256 devices in a mesh: datb: 8 (over z), model: 4 (over y), data: 8 (over x, core).
Axes of the slice: x: 4, y: 4, z: 8, core: 2. Of those that a mesh axis runs over, the one named last changes fastest.
Arguments:
- tokens: bfloat16 [16384, 2048], P(('datb', 'data', 'model'))
- w_gate: bfloat16 [2048, 16384], P(('datb', 'data'), 'model')
- w_up: bfloat16 [2048, 16384], P(('datb', 'data'), 'model')
- w_down: bfloat16 [16384, 2048], P('model', ('datb', 'data'))
- grad_out: bfloat16 [16384, 2048], P(('datb', 'data', 'model'))
Outputs:
- output 1: bfloat16 [16384, 2048], P(('datb', 'data', 'model'))
- output 2: bfloat16 [16384, 2048], P(('datb', 'data', 'model'))
- output 3: float32 [2048, 16384], P(('datb', 'data'), 'model')
- output 4: float32 [2048, 16384], P(('datb', 'data'), 'model')
- output 5: float32 [16384, 2048], P('model', ('datb', 'data'))
All inputs are finite; a program needn't handle non-finite values.
Results may differ from the reference program's by a relative error of at most 0.02.
Values are sent between devices in bfloat16 or wider.
A program may use at most 768 MiB of HBM per device.

```python
import jax
import jax.numpy as jnp
from jax import lax

D_MODEL = 2048
D_FF = 16384
TOKENS = 16384
BLOCK_ROWS = 512


def setup_inputs(seed: int = 0) -> dict:
    key = jax.random.key(seed)
    k_tok, k_gate, k_up, k_down, k_grad = jax.random.split(key, 5)
    tokens = jax.random.normal(k_tok, (TOKENS, D_MODEL), jnp.float32)
    w_gate = jax.random.normal(k_gate, (D_MODEL, D_FF), jnp.float32) * (D_MODEL ** -0.5)
    w_up = jax.random.normal(k_up, (D_MODEL, D_FF), jnp.float32) * (D_MODEL ** -0.5)
    w_down = jax.random.normal(k_down, (D_FF, D_MODEL), jnp.float32) * (1.5 * D_FF ** -0.5)
    grad_out = jax.random.normal(k_grad, (TOKENS, D_MODEL), jnp.float32)
    return {"tokens": tokens.astype(jnp.bfloat16), "w_gate": w_gate.astype(jnp.bfloat16), "w_up": w_up.astype(jnp.bfloat16), "w_down": w_down.astype(jnp.bfloat16), "grad_out": grad_out.astype(jnp.bfloat16)}


def block_pass(tok_rows, grad_rows, w_gate, w_up, w_down):
    gate_pre = jnp.dot(tok_rows, w_gate, preferred_element_type=jnp.float32).astype(jnp.bfloat16).astype(jnp.float32)
    up_pre = jnp.dot(tok_rows, w_up, preferred_element_type=jnp.float32).astype(jnp.bfloat16).astype(jnp.float32)
    gate_sig = jax.nn.sigmoid(gate_pre)
    silu_gate = gate_pre * gate_sig
    hidden = (silu_gate * up_pre).astype(jnp.bfloat16)
    down_out = jnp.dot(hidden, w_down, preferred_element_type=jnp.float32)
    out_rows = (tok_rows.astype(jnp.float32) + down_out).astype(jnp.bfloat16)
    grad_hidden = jnp.dot(grad_rows, w_down.T, preferred_element_type=jnp.float32).astype(jnp.bfloat16).astype(jnp.float32)
    grad_gate_pre = (grad_hidden * up_pre * gate_sig * (1.0 + gate_pre * (1.0 - gate_sig))).astype(jnp.bfloat16)
    grad_up_pre = (grad_hidden * silu_gate).astype(jnp.bfloat16)
    back_sum = jnp.dot(grad_gate_pre, w_gate.T, preferred_element_type=jnp.float32) + jnp.dot(grad_up_pre, w_up.T, preferred_element_type=jnp.float32)
    grad_in = (grad_rows.astype(jnp.float32) + back_sum).astype(jnp.bfloat16)
    part_gate = jnp.dot(tok_rows.T, grad_gate_pre, preferred_element_type=jnp.float32)
    part_up = jnp.dot(tok_rows.T, grad_up_pre, preferred_element_type=jnp.float32)
    part_down = jnp.dot(hidden.T, grad_rows, preferred_element_type=jnp.float32)
    return out_rows, grad_in, part_gate, part_up, part_down


def reference(tokens, w_gate, w_up, w_down, grad_out):
    block_count = TOKENS // BLOCK_ROWS
    tok_blocks = tokens.reshape(block_count, BLOCK_ROWS, D_MODEL)
    grad_blocks = grad_out.reshape(block_count, BLOCK_ROWS, D_MODEL)

    def scan_step(acc_carry, block_pair):
        acc_gate, acc_up, acc_down = acc_carry
        tok_rows, grad_rows = block_pair
        out_rows, grad_in, part_gate, part_up, part_down = block_pass(tok_rows, grad_rows, w_gate, w_up, w_down)
        return (acc_gate + part_gate, acc_up + part_up, acc_down + part_down), (out_rows, grad_in)

    zero_acc = (jnp.zeros((D_MODEL, D_FF), jnp.float32), jnp.zeros((D_MODEL, D_FF), jnp.float32), jnp.zeros((D_FF, D_MODEL), jnp.float32))
    acc_final, row_outs = lax.scan(scan_step, zero_acc, (tok_blocks, grad_blocks))
    grad_gate, grad_up, grad_down = acc_final
    out_blocks, grad_in_blocks = row_outs
    return (out_blocks.reshape(TOKENS, D_MODEL), grad_in_blocks.reshape(TOKENS, D_MODEL), grad_gate, grad_up, grad_down)
```

```python
import jax
import jax.numpy as jnp
from jax import lax
from jax.sharding import PartitionSpec as P

ROW_SPEC = P(("datb", "data", "model"), None)
GATE_SPEC = P(("datb", "data"), "model")
DOWN_SPEC = P("model", ("datb", "data"))


def dot(lhs, rhs, ldim, rdim):
    return lax.dot_general(lhs, rhs, (((ldim,), (rdim,)), ((), ())), preferred_element_type=jnp.float32)


def solution(mesh):
    data_size = mesh.shape["data"]

    def local_step(tok_loc, wg_loc, wu_loc, wd_loc, grad_loc):
        d_part, f_part = wg_loc.shape
        f_own = f_part // data_size

        mine = jnp.stack([wg_loc, wu_loc, wd_loc.T]).reshape(3, d_part, data_size, f_own)
        mine = lax.all_to_all(mine, "data", 2, 1, tiled=False)
        mine = mine.reshape(3, d_part * data_size, f_own)

        tok = lax.all_gather(tok_loc, ("data", "model"), axis=0, tiled=True)
        gate_w = lax.all_gather(mine[0], "datb", axis=0, tiled=True)
        up_w = lax.all_gather(mine[1], "datb", axis=0, tiled=True)
        grad = lax.all_gather(grad_loc, ("data", "model"), axis=0, tiled=True)
        down_w = lax.all_gather(mine[2], "datb", axis=0, tiled=True)

        gate_pre = dot(tok, gate_w, 1, 0).astype(jnp.bfloat16).astype(jnp.float32)
        up_pre = dot(tok, up_w, 1, 0).astype(jnp.bfloat16).astype(jnp.float32)
        gate_sig = jax.nn.sigmoid(gate_pre)
        silu_gate = gate_pre * gate_sig
        hidden = (silu_gate * up_pre).astype(jnp.bfloat16)

        def home(part):
            moved = lax.psum_scatter(part, "datb", scatter_dimension=0, tiled=True)
            moved = moved.reshape(data_size, d_part, f_own)
            return lax.all_to_all(moved, "data", 0, 1, tiled=False).reshape(d_part, f_part)

        grad_down = home(dot(grad, hidden, 0, 0)).T
        grad_hidden = dot(grad, down_w, 1, 0).astype(jnp.bfloat16).astype(jnp.float32)
        grad_gate_pre = (grad_hidden * up_pre * gate_sig * (1.0 + gate_pre * (1.0 - gate_sig))).astype(jnp.bfloat16)
        grad_up_pre = (grad_hidden * silu_gate).astype(jnp.bfloat16)
        grad_gate = home(dot(tok, grad_gate_pre, 0, 0))
        grad_up = home(dot(tok, grad_up_pre, 0, 0))

        down_part = dot(hidden, down_w, 1, 1).astype(jnp.bfloat16)
        back_part = (dot(grad_gate_pre, gate_w, 1, 1) + dot(grad_up_pre, up_w, 1, 1)).astype(jnp.bfloat16)
        down_sum = lax.psum_scatter(down_part, ("data", "model"), scatter_dimension=0, tiled=True)
        back_sum = lax.psum_scatter(back_part, ("data", "model"), scatter_dimension=0, tiled=True)
        out = (tok_loc.astype(jnp.float32) + down_sum.astype(jnp.float32)).astype(jnp.bfloat16)
        grad_in = (grad_loc.astype(jnp.float32) + back_sum.astype(jnp.float32)).astype(jnp.bfloat16)
        return out, grad_in, grad_gate, grad_up, grad_down

    return jax.shard_map(local_step, mesh=mesh, in_specs=(ROW_SPEC, GATE_SPEC, GATE_SPEC, DOWN_SPEC, ROW_SPEC), out_specs=(ROW_SPEC, ROW_SPEC, GATE_SPEC, GATE_SPEC, DOWN_SPEC), check_vma=False)
```

```python
import functools

import jax
import jax.numpy as jnp
from jax import lax
from jax.experimental import pallas as pl
from jax.experimental.pallas import tpu as pltpu
from jax.sharding import PartitionSpec as P

ROW_SPEC = P(("datb", "data", "model"), None)
GATE_SPEC = P(("datb", "data"), "model")
DOWN_SPEC = P("model", ("datb", "data"))
BF = jnp.bfloat16
F32 = jnp.float32
CORES = 2


def dot(lhs, rhs, ldim, rdim):
    return lax.dot_general(lhs, rhs, (((ldim,), (rdim,)), ((), ())), preferred_element_type=F32)


def sized(start, size):
    return pl.ds(pl.multiple_of(start, size), size)


def kernel(nz, ny, nx, tok_in, grad_in, wg_in, wu_in, wd_in, out_ref, gin_ref, dg_ref, du_ref, dd_ref,
           tok, grd, wgt, act, act_t, zrecv, zsend, ysum, stage, ya_recv, xa_recv, yb_recv, xb_recv,
           in_sem, a2a_s, a2a_r, ag_s, ag_r, p1_s, p1_r, p2_s, p2_r, pc_s, pc_r, rs_s, rs_r, credit,
           ex_s, ex_r, sa_s, sa_r, sb_s, sb_r, fa_s, fa_r):
    z, y, me = lax.axis_index("datb"), lax.axis_index("model"), lax.axis_index("data")
    x, c = me // CORES, lax.rem(me, CORES)
    nd = nx * CORES
    r, d_model = tok_in.shape
    dp, fp = wg_in.shape
    fo = fp // nd
    hf, zb, br = fo // 2, dp * nd, r * ny
    bh, rh = br // 2, r // 2

    z_to = ({"datb": lax.rem(z + 1, nz)}, {"datb": lax.rem(z + nz - 1, nz)})
    y_to = ({"model": lax.rem(y + 1, ny)}, {"model": lax.rem(y + ny - 1, ny)})
    x_to = ({"data": lax.rem(x + 1, nx) * CORES + c}, {"data": lax.rem(x + nx - 1, nx) * CORES + c})
    mate = {"data": x * CORES + 1 - c}

    def back(pos, n, d, s):
        return lax.rem(pos - s + 2 * n, n) if d == 0 else lax.rem(pos + s, n)

    def rcopy(src, dst, ss, rs, to):
        return pltpu.make_async_remote_copy(src_ref=src, dst_ref=dst, send_sem=ss, recv_sem=rs, device_id=to,
                                            device_id_type=pl.DeviceIdType.MESH)

    own = (tok.at[x, c, sized(y * r, r), :], grd.at[x, c, sized(y * r, r), :])
    w_in = (wg_in, wu_in, wd_in)
    moves = list(zip((tok_in, grad_in), own))
    moves += [(w_in[m].at[:, sized(me * fo, fo)], wgt.at[m, sized(z * zb + me * dp, dp), :]) for m in range(3)]
    loads = [pltpu.make_async_copy(src, dst, in_sem.at[i]) for i, (src, dst) in enumerate(moves)]
    for cp in loads:
        cp.start()
    barrier = pltpu.get_barrier_semaphore()
    peers = [{"data": lax.rem(me + k, nd)} for k in range(1, nd)]
    for to in peers + list(z_to) + list(y_to):
        pl.semaphore_signal(barrier, inc=1, device_id=to, device_id_type=pl.DeviceIdType.MESH)
    pl.semaphore_wait(barrier, nd - 1 + 4)

    def a2a(m, k):
        to = lax.rem(me + k, nd)
        return rcopy(w_in[m].at[:, sized(to * fo, fo)], wgt.at[m, sized(z * zb + me * dp, dp), :],
                     a2a_s.at[m, k - 1], a2a_r.at[m, k - 1], {"data": to})

    def a2a_wait(m, k):
        frm = lax.rem(me + nd - k, nd)
        dst = wgt.at[m, sized(z * zb + frm * dp, dp), :]
        rcopy(dst, dst, a2a_s.at[m, k - 1], a2a_r.at[m, k - 1], {"data": frm}).wait_recv()

    def ag_copy(m, d, s, pos):
        ref = wgt.at[m, sized(back(pos, nz, d, s) * zb, zb), pl.ds(d * hf, hf)]
        return rcopy(ref, ref, ag_s.at[m, d, s], ag_r.at[m, d, s], z_to[d])

    def ag_send(m, d, s):
        ag_copy(m, d, s, z).start()

    def ag_wait(m, d, s):
        ag_copy(m, d, s, z - 1 if d == 0 else z + 1).wait_recv()

    def p1_copy(arr, d, s, shift):
        if arr == 0:
            pos = y + shift
            ref = tok.at[x, c, sized(back(pos, ny, d, s) * r + d * rh, rh), :]
        else:
            pos = x + shift
            ref = grd.at[back(pos, nx, d, s), c, sized(y * r + d * rh, rh), :]
        return rcopy(ref, ref, p1_s.at[arr, d, s], p1_r.at[arr, d, s], (y_to, x_to)[arr][d])

    def p2_ref(arr, d, blk):
        if arr == 0:
            return tok.at[blk, c, pl.ds(d * bh, bh), :]
        return grd.at[:, c, sized(blk * r + d * rh, rh), :]

    def p2_copy(arr, d, s, shift):
        pos, n = ((x, nx), (y, ny))[arr]
        ref = p2_ref(arr, d, back(pos + shift, n, d, s))
        return rcopy(ref, ref, p2_s.at[arr, d, s], p2_r.at[arr, d, s], (x_to, y_to)[arr][d])

    def shift_of(d):
        return -1 if d == 0 else 1

    p1_n, p2_n = (ny - 1, nx - 1), (nx - 1, ny - 1)
    def pc_copy(arr, idx, core):
        if idx == 0:
            ref = tok.at[x, core] if arr == 0 else grd.at[:, core, sized(y * r, r), :]
        else:
            s, d = (idx - 1) // 2, (idx - 1) % 2
            pos, n = ((x, nx), (y, ny))[arr]
            blk = back(pos + shift_of(d), n, d, s)
            ref = tok.at[blk, core, pl.ds(d * bh, bh), :] if arr == 0 else grd.at[:, core, sized(blk * r + d * rh, rh), :]
        return rcopy(ref, ref, pc_s.at[arr, idx], pc_r.at[arr, idx], mate)

    def p1_event(s):
        for arr in (0, 1):
            for d in (0, 1):
                if 0 < s <= p1_n[arr]:
                    p1_copy(arr, d, s - 1, shift_of(d)).wait_recv()
                if s < p1_n[arr]:
                    p1_copy(arr, d, s, 0).start()

    def p2_event(s):
        for arr in (0, 1):
            for d in (0, 1):
                if 0 < s <= p2_n[arr]:
                    p2_copy(arr, d, s - 1, shift_of(d)).wait_recv()
                if s < p2_n[arr]:
                    p2_copy(arr, d, s, 0).start()
                if 0 < s <= p2_n[arr]:
                    pc_copy(arr, 1 + 2 * (s - 1) + d, c).start()
            if s == 0:
                pc_copy(arr, 0, c).start()

    def z_event(s):
        for m in range(3):
            for d in (0, 1):
                if s > 0:
                    ag_wait(m, d, s - 1)
                if s < nz - 1:
                    ag_send(m, d, s)

    for k in range(1, nd):
        a2a(0, k).start()
    for cp in loads:
        cp.wait()
    p1_event(0)
    for m in (1, 2):
        for k in range(1, nd):
            a2a(m, k).start()
    p1_event(1)
    for m in range(3):
        for k in range(1, nd):
            a2a_wait(m, k)
        for d in (0, 1):
            ag_send(m, d, 0)
    p1_last, p2_last = max(p1_n), max(p2_n)
    for s in range(2, p1_last + 1):
        p1_event(s)
    p2_at = {0: 0.0}
    for s in range(1, p2_last + 1):
        p2_at[s] = s * 11.5
    marks = [(p2_at[s], 0, s) for s in p2_at] + [(4.0 + 8.2 * (s - 1), 1, s) for s in range(1, nz)]
    for _, kind, s in sorted(marks):
        (p2_event, z_event)[kind](s)
    for arr in (0, 1):
        for idx in range(1 + 2 * p2_n[arr]):
            pc_copy(arr, idx, 1 - c).wait_recv()

    def act_block(t, carry):
        i, half = t // 2, lax.rem(t, 2)
        sl = sized(half * hf, hf)
        xi, ci = i // CORES, lax.rem(i, CORES)
        x_rows, g_rows = tok[xi, ci], grd[xi, ci]
        gate_pre = dot(x_rows, wgt[0, :, sl], 1, 0).astype(BF).astype(F32)
        up_pre = dot(x_rows, wgt[1, :, sl], 1, 0).astype(BF).astype(F32)
        grad_h = dot(g_rows, wgt[2, :, sl], 1, 0).astype(BF).astype(F32)
        sig = jax.nn.sigmoid(gate_pre)
        silu = gate_pre * sig
        vals = ((grad_h * up_pre * sig * (1.0 + gate_pre * (1.0 - sig))).astype(BF), (grad_h * silu).astype(BF), (silu * up_pre).astype(BF))
        for m in range(3):
            act[m, i, :, sl] = vals[m]
            act_t[m, sl, sized(i * br, br)] = vals[m].T
        return carry

    lax.fori_loop(0, nd * 2, act_block, 0)

    outs = (dg_ref, du_ref, dd_ref)

    def part(m, d, blk):
        src = grd if m == 2 else tok
        rhs = src[:, :, :, sized(blk * zb, zb)].reshape(nd * br, zb)
        return dot(act_t[m, pl.ds(d * hf, hf), :], rhs, 1, 0)

    def rs_copy(m, d, s):
        slot = lax.rem(s, 2)
        return rcopy(zsend.at[m, d, slot], zrecv.at[m, d, slot], rs_s.at[m, d, s], rs_r.at[m, d, s], z_to[d])

    def rs_step(s, first):
        for m in range(3):
            for d in (0, 1):
                blk = lax.rem(z - 1 - s + 2 * nz, nz) if d == 0 else lax.rem(z + 1 + s, nz)
                val = part(m, d, blk)
                if not first:
                    rs_copy(m, d, s - 1).wait_recv()
                    val = val + zrecv[m, d, lax.rem(s - 1, 2)]

                    @pl.when(s >= 2)
                    def _():
                        rs_copy(m, d, s - 2).wait_send()

                zsend[m, d, lax.rem(s, 2)] = val
                if not first:

                    @pl.when(s <= nz - 3)
                    def _():
                        pl.semaphore_signal(credit.at[m, d], inc=1, device_id=z_to[1 - d], device_id_type=pl.DeviceIdType.MESH)

                    @pl.when(s >= 2)
                    def _():
                        pl.semaphore_wait(credit.at[m, d], 1)

                rs_copy(m, d, s).start()

    rs_step(0, True)

    cols = d_model // 4

    def ex_copy(arr, xi):
        return rcopy(stage.at[arr], ysum.at[arr, xi], ex_s.at[arr, xi], ex_r.at[arr, xi], mate)

    def row_part(arr, i, j):
        sl = sized(j * cols, cols)
        if arr == 0:
            return dot(act[2, i], wgt[2, sl, :], 1, 1)
        return dot(act[0, i], wgt[0, sl, :], 1, 1) + dot(act[1, i], wgt[1, sl, :], 1, 1)

    def give(xi, carry):
        for arr in (0, 1):

            @pl.when(xi >= 1)
            def _():
                ex_copy(arr, xi - 1).wait_send()

            def fill(j, carry):
                stage[arr, :, sized(j * cols, cols)] = row_part(arr, xi * CORES + 1 - c, j).astype(BF)
                return carry

            lax.fori_loop(0, d_model // cols, fill, 0)
            ex_copy(arr, xi).start()
        return carry

    lax.fori_loop(0, nx, give, 0)

    def keep(xi, carry):
        for arr in (0, 1):
            ex_copy(arr, xi).wait_recv()

            def fill(j, carry):
                sl = sized(j * cols, cols)
                mine = row_part(arr, xi * CORES + c, j).astype(BF).astype(F32)
                ysum[arr, xi, :, sl] = (mine + ysum[arr, xi, :, sl].astype(F32)).astype(BF)
                return carry

            lax.fori_loop(0, d_model // cols, fill, 0)
        return carry

    lax.fori_loop(0, nx, keep, 0)

    sa_n, sb_n = (nx - 1, ny - 1), (ny - 1, nx - 1)
    recv_a, recv_b = (ya_recv, xa_recv), (yb_recv, xb_recv)

    def sa_ref(arr, d, blk):
        if arr == 0:
            return ysum.at[0, blk, pl.ds(d * bh, bh), :]
        return ysum.at[1, :, sized(blk * r + d * rh, rh), :]

    def sb_ref(arr, d, blk):
        if arr == 0:
            return ysum.at[0, x, sized(blk * r + d * rh, rh), :]
        return ysum.at[1, blk, sized(y * r + d * rh, rh), :]

    def add_into(ref, slot):
        flat = len(ref.shape) == 2
        count = ref.shape[0] // 16 if flat else ref.shape[0]

        def piece(i, carry):
            at = sized(i * 16, 16) if flat else i
            ref[at] = (ref[at].astype(F32) + slot[at].astype(F32)).astype(BF)
            return carry

        lax.fori_loop(0, count, piece, 0)

    def scatter_event(refs, counts, recv, ss, rr, to, pos, s, last):
        for arr in (0, 1):
            n = counts[arr] + 1
            if s > counts[arr]:
                continue
            for d in (0, 1):
                blk = back(pos[arr] + shift_of(d), n, d, s)
                ref = refs(arr, d, blk)
                if s > 0:
                    slot = recv[arr].at[d, s - 1]
                    rcopy(slot, slot, ss.at[arr, d, s - 1], rr.at[arr, d, s - 1], to[arr][d]).wait_recv()
                    add_into(ref, slot)
                if s < counts[arr]:
                    rcopy(ref, recv[arr].at[d, s], ss.at[arr, d, s], rr.at[arr, d, s], to[arr][d]).start()

    def sa_event(s):
        scatter_event(sa_ref, sa_n, recv_a, sa_s, sa_r, (x_to, y_to), (x, y), s, False)

    def sb_event(s):
        scatter_event(sb_ref, sb_n, recv_b, sb_s, sb_r, (y_to, x_to), (y, x), s, True)

    def sb_finish():
        for arr, dst in ((0, out_ref), (1, gin_ref)):
            total = ysum[arr, x, sized(y * r, r), :].astype(F32)
            dst[...] = (own[arr][...].astype(F32) + total).astype(BF)

    sa_event(0)
    steps = [[functools.partial(sa_event, s)] for s in range(1, max(sa_n) + 1)]
    steps[-1].append(functools.partial(sb_event, 0))
    steps += [[functools.partial(sb_event, s)] for s in range(1, max(sb_n) + 1)]
    steps[-1].append(sb_finish)

    def ring(s, carry):
        rs_step(s, False)
        for k, fs in enumerate(steps[: nz - 2]):

            @pl.when(s == k + 1)
            def _(fs=fs):
                for f in fs:
                    f()

        return carry

    lax.fori_loop(1, nz - 1, ring, 0)
    for fs in steps[nz - 2:]:
        for f in fs:
            f()

    spare = (nz - 1) % 2

    def fin_copy(m, d, k):
        to = lax.rem(me + k, nd)
        return rcopy(zsend.at[m, d, spare, sized(to * dp, dp), :], outs[m].at[:, sized(me * fo + d * hf, hf)],
                     fa_s.at[m, d, k - 1], fa_r.at[m, d, k - 1], {"data": to})

    for m in range(3):
        for d in (0, 1):
            val = part(m, d, z)
            rs_copy(m, d, nz - 2).wait_recv()
            rs_copy(m, d, nz - 3).wait_send()
            zsend[m, d, spare] = (val + zrecv[m, d, nz % 2]).T
            for k in range(1, nd):
                fin_copy(m, d, k).start()
            outs[m][:, sized(me * fo + d * hf, hf)] = zsend[m, d, spare, sized(me * dp, dp), :]

    for m in range(3):
        for k in range(1, nd):
            frm = lax.rem(me + nd - k, nd)
            for d in (0, 1):
                dst = outs[m].at[:, sized(frm * fo + d * hf, hf)]
                rcopy(dst, dst, fa_s.at[m, d, k - 1], fa_r.at[m, d, k - 1], {"data": frm}).wait_recv()
                fin_copy(m, d, k).wait_send()
            a2a(m, k).wait_send()
        for d in (0, 1):
            for s in range(nz - 1):
                ag_copy(m, d, s, z).wait_send()
            rs_copy(m, d, nz - 2).wait_send()
    for arr in (0, 1):
        for d in (0, 1):
            for s in range(p1_n[arr]):
                p1_copy(arr, d, s, 0).wait_send()
            for s in range(p2_n[arr]):
                p2_copy(arr, d, s, 0).wait_send()
            for s in range(sa_n[arr]):
                ref = recv_a[arr].at[d, s]
                rcopy(ref, ref, sa_s.at[arr, d, s], sa_r.at[arr, d, s], z_to[0]).wait_send()
            for s in range(sb_n[arr]):
                ref = recv_b[arr].at[d, s]
                rcopy(ref, ref, sb_s.at[arr, d, s], sb_r.at[arr, d, s], z_to[0]).wait_send()
        for idx in range(1 + 2 * p2_n[arr]):
            pc_copy(arr, idx, c).wait_send()
        ex_copy(arr, nx - 1).wait_send()


def solution(mesh):
    nz, ny, nd = mesh.shape["datb"], mesh.shape["model"], mesh.shape["data"]
    nx = nd // CORES

    def local_step(tok_loc, wg_loc, wu_loc, wd_loc, grad_loc):
        r, d_model = tok_loc.shape
        dp, fp = wg_loc.shape
        fo = fp // nd
        hf, zb, br = fo // 2, dp * nd, r * ny
        bh, rh = br // 2, r // 2
        vmem = pl.BlockSpec(memory_space=pltpu.VMEM)
        hbm = pl.BlockSpec(memory_space=pl.ANY)
        dma = pltpu.SemaphoreType.DMA
        most = max(nx, ny) - 1
        out, gin, dg, du, dd = pl.pallas_call(
            functools.partial(kernel, nz, ny, nx),
            out_shape=[jax.ShapeDtypeStruct((r, d_model), BF)] * 2 + [jax.ShapeDtypeStruct((dp, fp), F32)] * 3,
            in_specs=[hbm] * 5,
            out_specs=[vmem] * 5,
            scratch_shapes=[
                pltpu.VMEM((nx, CORES, br, d_model), BF),
                pltpu.VMEM((nx, CORES, br, d_model), BF),
                pltpu.VMEM((3, d_model, fo), BF),
                pltpu.VMEM((3, nd, br, fo), BF),
                pltpu.VMEM((3, fo, nd * br), BF),
                pltpu.VMEM((3, 2, 2, hf, zb), F32),
                pltpu.VMEM((3, 2, 2, hf, zb), F32),
                pltpu.VMEM((2, nx, br, d_model), BF),
                pltpu.VMEM((2, br, d_model), BF),
                pltpu.VMEM((2, nx - 1, bh, d_model), BF),
                pltpu.VMEM((2, ny - 1, nx, rh, d_model), BF),
                pltpu.VMEM((2, ny - 1, rh, d_model), BF),
                pltpu.VMEM((2, nx - 1, rh, d_model), BF),
                dma((5,)),
                dma((3, nd - 1)), dma((3, nd - 1)),
                dma((3, 2, nz - 1)), dma((3, 2, nz - 1)),
                dma((2, 2, most)), dma((2, 2, most)),
                dma((2, 2, most)), dma((2, 2, most)),
                dma((2, 1 + 2 * most)), dma((2, 1 + 2 * most)),
                dma((3, 2, nz - 1)), dma((3, 2, nz - 1)),
                pltpu.SemaphoreType.REGULAR((3, 2)),
                dma((2, nx)), dma((2, nx)),
                dma((2, 2, most)), dma((2, 2, most)),
                dma((2, 2, most)), dma((2, 2, most)),
                dma((3, 2, nd - 1)), dma((3, 2, nd - 1)),
            ],
            compiler_params=pltpu.CompilerParams(collective_id=0, has_side_effects=True, vmem_limit_bytes=67043328),
            name="swiglu_step",
        )(tok_loc, grad_loc, wg_loc, wu_loc, wd_loc.T)
        return out, gin, dg, du, dd.T

    return jax.shard_map(local_step, mesh=mesh, in_specs=(ROW_SPEC, GATE_SPEC, GATE_SPEC, DOWN_SPEC, ROW_SPEC), out_specs=(ROW_SPEC, ROW_SPEC, GATE_SPEC, GATE_SPEC, DOWN_SPEC), check_vma=False)
```

```python
import functools

import jax
import jax.numpy as jnp
from jax import lax
from jax.experimental import pallas as pl
from jax.experimental.pallas import tpu as pltpu
from jax.sharding import PartitionSpec as P

ROW_SPEC = P(("datb", "data", "model"), None)
GATE_SPEC = P(("datb", "data"), "model")
DOWN_SPEC = P("model", ("datb", "data"))
BF = jnp.bfloat16
F32 = jnp.float32
CORES = 2


def dot(lhs, rhs, ldim, rdim):
    return lax.dot_general(lhs, rhs, (((ldim,), (rdim,)), ((), ())), preferred_element_type=F32)


def sized(start, size):
    return pl.ds(pl.multiple_of(start, size), size)


def kernel(nz, ny, nx, tok_in, grad_in, wg_in, wu_in, wd_in, out_ref, gin_ref, dg_ref, du_ref, dd_ref,
           tok, grd, wgt, act, act_t, zrecv, zsend, ysum, stage, ya_recv, xa_recv, yb_recv, xb_recv,
           in_sem, a2a_s, a2a_r, ag_s, ag_r, p1_s, p1_r, p2_s, p2_r, pc_s, pc_r, rs_s, rs_r, credit,
           ex_s, ex_r, sa_s, sa_r, sb_s, sb_r, fa_s, fa_r):
    z, y, me = lax.axis_index("datb"), lax.axis_index("model"), lax.axis_index("data")
    x, c = me // CORES, lax.rem(me, CORES)
    nd = nx * CORES
    r, d_model = tok_in.shape
    dp, fp = wg_in.shape
    fo = fp // nd
    hf, zb, br = fo // 2, dp * nd, r * ny
    bh, rh = br // 2, r // 2

    z_to = ({"datb": lax.rem(z + 1, nz)}, {"datb": lax.rem(z + nz - 1, nz)})
    y_to = ({"model": lax.rem(y + 1, ny)}, {"model": lax.rem(y + ny - 1, ny)})
    x_to = ({"data": lax.rem(x + 1, nx) * CORES + c}, {"data": lax.rem(x + nx - 1, nx) * CORES + c})
    mate = {"data": x * CORES + 1 - c}

    def back(pos, n, d, s):
        return lax.rem(pos - s + 2 * n, n) if d == 0 else lax.rem(pos + s, n)

    def rcopy(src, dst, ss, rs, to):
        return pltpu.make_async_remote_copy(src_ref=src, dst_ref=dst, send_sem=ss, recv_sem=rs, device_id=to,
                                            device_id_type=pl.DeviceIdType.MESH)

    own = (tok.at[x, c, sized(y * r, r), :], grd.at[x, c, sized(y * r, r), :])
    w_in = (wg_in, wu_in, wd_in)
    moves = list(zip((tok_in, grad_in), own))
    moves += [(w_in[m].at[:, sized(me * fo, fo)], wgt.at[m, sized(z * zb + me * dp, dp), :]) for m in range(3)]
    loads = [pltpu.make_async_copy(src, dst, in_sem.at[i]) for i, (src, dst) in enumerate(moves)]
    for cp in loads:
        cp.start()
    barrier = pltpu.get_barrier_semaphore()
    peers = [{"data": lax.rem(me + k, nd)} for k in range(1, nd)]
    for to in peers + list(z_to) + list(y_to):
        pl.semaphore_signal(barrier, inc=1, device_id=to, device_id_type=pl.DeviceIdType.MESH)
    pl.semaphore_wait(barrier, nd - 1 + 4)

    def a2a(m, k):
        to = lax.rem(me + k, nd)
        return rcopy(w_in[m].at[:, sized(to * fo, fo)], wgt.at[m, sized(z * zb + me * dp, dp), :],
                     a2a_s.at[m, k - 1], a2a_r.at[m, k - 1], {"data": to})

    def a2a_wait(m, k):
        frm = lax.rem(me + nd - k, nd)
        dst = wgt.at[m, sized(z * zb + frm * dp, dp), :]
        rcopy(dst, dst, a2a_s.at[m, k - 1], a2a_r.at[m, k - 1], {"data": frm}).wait_recv()

    streams = ((0, 0, zb), (1, 0, zb), (2, 0, zb // 2), (2, zb // 2, zb // 2))

    def ag_copy(q, d, s, ahead):
        m, first, rows = streams[q]
        ref = wgt.at[m, sized(back(z, nz, d, s + ahead) * zb + first, rows), pl.ds(d * hf, hf)]
        return rcopy(ref, ref, ag_s.at[q, d, s], ag_r.at[q, d, s], z_to[d])

    def z_event(m, s):
        for q in range(4):
            if streams[q][0] == m:
                for d in (0, 1):
                    if s > 0:
                        ag_copy(q, d, s - 1, 1).wait_recv()
                    if s < nz - 1:
                        ag_copy(q, d, s, 0).start()

    first_n, second_n = (ny, nx), (nx, ny)
    first_to, second_to = (y_to, x_to), (x_to, y_to)

    def cell(arr, j, t, h, core):
        if arr == 0:
            return tok.at[back(x, nx, h, t), core, sized(back(y, ny, h, j) * r + h * rh, rh), :]
        return grd.at[back(x, nx, h, j), core, sized(back(y, ny, h, t) * r + h * rh, rh), :]

    def p1_copy(arr, h, j, ahead):
        ref = cell(arr, j + ahead, 0, h, c)
        return rcopy(ref, ref, p1_s.at[arr, h, j], p1_r.at[arr, h, j], first_to[arr][h])

    def p2_copy(arr, h, j, t, ahead):
        ref = cell(arr, j, t + ahead, h, c)
        return rcopy(ref, ref, p2_s.at[arr, h, j, t], p2_r.at[arr, h, j, t], second_to[arr][h])

    def pc_copy(arr, h, j, t, core):
        ref = cell(arr, j, t, h, core)
        return rcopy(ref, ref, pc_s.at[arr, h, j, t], pc_r.at[arr, h, j, t], mate)

    def token_event(j, t):
        for arr in (0, 1):
            if j < first_n[arr] and t < second_n[arr]:
                for h in (0, 1):
                    if t > 0:
                        p2_copy(arr, h, j, t - 1, 1).wait_recv()
                    elif j > 0:
                        p1_copy(arr, h, j - 1, 1).wait_recv()
                    if t == 0 and j < first_n[arr] - 1:
                        p1_copy(arr, h, j, 0).start()
                    if t < second_n[arr] - 1:
                        p2_copy(arr, h, j, t, 0).start()
                    pc_copy(arr, h, j, t, c).start()

    def a2a_event(m):
        for k in range(1, nd):
            a2a_wait(m, k)
        z_event(m, 0)

    for m in range(3):
        for k in range(1, nd):
            a2a(m, k).start()
    for cp in loads:
        cp.wait()

    most = max(nx, ny)
    marks = []
    sends = 0
    for ready, j, t in sorted((4.2 * j + 5.4 * t, j, t) for j in range(most) for t in range(most)):
        marks.append((10.0 * (j + t > 0) + max(ready, 3.4 * sends), len(marks), functools.partial(token_event, j, t)))
        sends += t < most - 1
    for m in range(3):
        marks.append((5.0 + 2.0 * m, len(marks), functools.partial(a2a_event, m)))
    ring_order = [(m, s) for s in range(1, nz) for m in (0, 1, 2)[: 3 if s % 2 == 0 else 2]]
    ring_order = [(m, s if m < 2 else s // 2) for m, s in ring_order]
    clock = 12.0
    for m, s in ring_order:
        marks.append((clock, len(marks), functools.partial(z_event, m, s)))
        clock += 2.8
    for _, _, f in sorted(marks, key=lambda mark: mark[:2]):
        f()
    late = [s for s in range(1, nz) if (2, s) not in ring_order]
    for arr in (0, 1):
        for h in (0, 1):
            for j in range(first_n[arr]):
                for t in range(second_n[arr]):
                    pc_copy(arr, h, j, t, 1 - c).wait_recv()

    def blocks(t):
        i, half = t // 2, lax.rem(t, 2)
        return i, i // CORES, lax.rem(i, CORES), sized(half * hf, hf)

    def forward_block(t, carry):
        i, xi, ci, sl = blocks(t)
        x_rows = tok[xi, ci]
        gate_b = dot(x_rows, wgt[0, :, sl], 1, 0).astype(BF)
        up_b = dot(x_rows, wgt[1, :, sl], 1, 0).astype(BF)
        gate_pre, up_pre = gate_b.astype(F32), up_b.astype(F32)
        hidden = (gate_pre * jax.nn.sigmoid(gate_pre) * up_pre).astype(BF)
        act[0, i, :, sl] = gate_b
        act[1, i, :, sl] = up_b
        act[2, i, :, sl] = hidden
        act_t[2, sl, sized(i * br, br)] = hidden.T
        for n, s in enumerate(late):

            @pl.when(t == (n + 1) * 2 * nd // len(late) - 1)
            def _():
                z_event(2, s)

        return carry

    lax.fori_loop(0, nd * 2, forward_block, 0)

    def backward_block(t, carry):
        i, xi, ci, sl = blocks(t)
        gate_pre, up_pre = act[0, i, :, sl].astype(F32), act[1, i, :, sl].astype(F32)
        grad_h = dot(grd[xi, ci], wgt[2, :, sl], 1, 0).astype(BF).astype(F32)
        sig = jax.nn.sigmoid(gate_pre)
        vals = ((grad_h * up_pre * sig * (1.0 + gate_pre * (1.0 - sig))).astype(BF), (grad_h * (gate_pre * sig)).astype(BF))
        for m in range(2):
            act[m, i, :, sl] = vals[m]
            act_t[m, sl, sized(i * br, br)] = vals[m].T
        return carry

    outs = (dg_ref, du_ref, dd_ref)

    def part(m, d, blk):
        src = grd if m == 2 else tok
        rhs = src[:, :, :, sized(blk * zb, zb)].reshape(nd * br, zb)
        return dot(act_t[m, pl.ds(d * hf, hf), :], rhs, 1, 0)

    def rs_copy(m, d, s):
        slot = lax.rem(s, 2)
        return rcopy(zsend.at[m, d, slot], zrecv.at[m, d, slot], rs_s.at[m, d, s], rs_r.at[m, d, s], z_to[d])

    def shift_of(d):
        return -1 if d == 0 else 1

    def rs_chunk(m, s, first):
        for d in (0, 1):
            blk = lax.rem(z - 1 - s + 2 * nz, nz) if d == 0 else lax.rem(z + 1 + s, nz)
            val = part(m, d, blk)
            if not first:
                rs_copy(m, d, s - 1).wait_recv()
                val = val + zrecv[m, d, lax.rem(s - 1, 2)]

                @pl.when(s >= 2)
                def _():
                    rs_copy(m, d, s - 2).wait_send()

            zsend[m, d, lax.rem(s, 2)] = val
            if not first:

                @pl.when(s <= nz - 3)
                def _():
                    pl.semaphore_signal(credit.at[m, d], inc=1, device_id=z_to[1 - d], device_id_type=pl.DeviceIdType.MESH)

                @pl.when(s >= 2)
                def _():
                    pl.semaphore_wait(credit.at[m, d], 1)

            rs_copy(m, d, s).start()

    order = (2, 0, 1)
    rs_chunk(2, 0, True)
    lax.fori_loop(0, nd * 2, backward_block, 0)

    cols = d_model // 4

    def ex_copy(arr, xi):
        return rcopy(stage.at[arr], ysum.at[arr, xi], ex_s.at[arr, xi], ex_r.at[arr, xi], mate)

    def row_part(arr, i, j):
        sl = sized(j * cols, cols)
        if arr == 0:
            return dot(act[2, i], wgt[2, sl, :], 1, 1)
        return dot(act[0, i], wgt[0, sl, :], 1, 1) + dot(act[1, i], wgt[1, sl, :], 1, 1)

    def give(xi):
        for arr in (0, 1):
            if xi >= 1:
                ex_copy(arr, xi - 1).wait_send()

            def fill(j, carry):
                stage[arr, :, sized(j * cols, cols)] = row_part(arr, xi * CORES + 1 - c, j).astype(BF)
                return carry

            lax.fori_loop(0, d_model // cols, fill, 0)
            ex_copy(arr, xi).start()

    def keep(xi):
        for arr in (0, 1):
            ex_copy(arr, xi).wait_recv()

            def fill(j, carry):
                sl = sized(j * cols, cols)
                mine = row_part(arr, xi * CORES + c, j).astype(BF).astype(F32)
                ysum[arr, xi, :, sl] = (mine + ysum[arr, xi, :, sl].astype(F32)).astype(BF)
                return carry

            lax.fori_loop(0, d_model // cols, fill, 0)

    sa_n, sb_n = (nx - 1, ny - 1), (ny - 1, nx - 1)
    recv_a, recv_b = (ya_recv, xa_recv), (yb_recv, xb_recv)

    def sa_ref(arr, d, blk):
        if arr == 0:
            return ysum.at[0, blk, pl.ds(d * bh, bh), :]
        return ysum.at[1, :, sized(blk * r + d * rh, rh), :]

    def sb_ref(arr, d, blk):
        if arr == 0:
            return ysum.at[0, x, sized(blk * r + d * rh, rh), :]
        return ysum.at[1, blk, sized(y * r + d * rh, rh), :]

    def add_into(ref, slot):
        flat = len(ref.shape) == 2
        count = ref.shape[0] // 16 if flat else ref.shape[0]

        def piece(i, carry):
            at = sized(i * 16, 16) if flat else i
            ref[at] = (ref[at].astype(F32) + slot[at].astype(F32)).astype(BF)
            return carry

        lax.fori_loop(0, count, piece, 0)

    def scatter_event(refs, counts, recv, ss, rr, to, pos, s, last):
        for arr in (0, 1):
            n = counts[arr] + 1
            if s > counts[arr]:
                continue
            for d in (0, 1):
                blk = back(pos[arr] + shift_of(d), n, d, s)
                ref = refs(arr, d, blk)
                if s > 0:
                    slot = recv[arr].at[d, s - 1]
                    rcopy(slot, slot, ss.at[arr, d, s - 1], rr.at[arr, d, s - 1], to[arr][d]).wait_recv()
                    add_into(ref, slot)
                if s < counts[arr]:
                    rcopy(ref, recv[arr].at[d, s], ss.at[arr, d, s], rr.at[arr, d, s], to[arr][d]).start()

    def sa_event(s):
        scatter_event(sa_ref, sa_n, recv_a, sa_s, sa_r, (x_to, y_to), (x, y), s, False)

    def sb_event(s):
        scatter_event(sb_ref, sb_n, recv_b, sb_s, sb_r, (y_to, x_to), (y, x), s, True)

    def sb_finish():
        for arr, dst in ((0, out_ref), (1, gin_ref)):
            total = ysum[arr, x, sized(y * r, r), :].astype(F32)
            dst[...] = (own[arr][...].astype(F32) + total).astype(BF)

    slots = 3 * (nz - 1)
    work = [functools.partial(give, xi) for xi in range(nx)] + [functools.partial(keep, xi) for xi in range(nx)]
    plan = list(enumerate(work, 1))
    at = 1 + len(work)
    for s in range(max(sa_n) + 1):
        plan.append((at + 3 * s, functools.partial(sa_event, s)))
    at += 3 * max(sa_n)
    for s in range(max(sb_n) + 1):
        plan.append((at + s, functools.partial(sb_event, s)))
    plan.append((at + max(sb_n), sb_finish))

    for idx in (1, 2):
        rs_chunk(order[idx], 0, True)
        for slot, f in plan:
            if slot == idx:
                f()

    def ring(s, carry):
        for idx, m in enumerate(order):
            rs_chunk(m, s, False)
            for k in range(1, nz - 1):
                fs = [f for slot, f in plan if slot == 3 * k + idx]
                if fs:

                    @pl.when(s == k)
                    def _():
                        for f in fs:
                            f()

        return carry

    lax.fori_loop(1, nz - 1, ring, 0)
    for slot, f in plan:
        if slot >= slots:
            f()

    spare = (nz - 1) % 2

    def fin_copy(m, d, k):
        to = lax.rem(me + k, nd)
        return rcopy(zsend.at[m, d, spare, sized(to * dp, dp), :], outs[m].at[:, sized(me * fo + d * hf, hf)],
                     fa_s.at[m, d, k - 1], fa_r.at[m, d, k - 1], {"data": to})

    for m in order:
        for d in (0, 1):
            val = part(m, d, z)
            rs_copy(m, d, nz - 2).wait_recv()
            rs_copy(m, d, nz - 3).wait_send()
            zsend[m, d, spare] = (val + zrecv[m, d, nz % 2]).T
            for k in range(1, nd):
                fin_copy(m, d, k).start()
            outs[m][:, sized(me * fo + d * hf, hf)] = zsend[m, d, spare, sized(me * dp, dp), :]

    for m in order:
        for k in range(1, nd):
            frm = lax.rem(me + nd - k, nd)
            for d in (0, 1):
                dst = outs[m].at[:, sized(frm * fo + d * hf, hf)]
                rcopy(dst, dst, fa_s.at[m, d, k - 1], fa_r.at[m, d, k - 1], {"data": frm}).wait_recv()
                fin_copy(m, d, k).wait_send()
            a2a(m, k).wait_send()
        for d in (0, 1):
            rs_copy(m, d, nz - 2).wait_send()
    for q in range(4):
        for d in (0, 1):
            for s in range(nz - 1):
                ag_copy(q, d, s, 0).wait_send()
    for arr in (0, 1):
        for h in (0, 1):
            for j in range(first_n[arr]):
                if j < first_n[arr] - 1:
                    p1_copy(arr, h, j, 0).wait_send()
                for t in range(second_n[arr]):
                    if t < second_n[arr] - 1:
                        p2_copy(arr, h, j, t, 0).wait_send()
                    pc_copy(arr, h, j, t, c).wait_send()
            for s in range(sa_n[arr]):
                ref = recv_a[arr].at[h, s]
                rcopy(ref, ref, sa_s.at[arr, h, s], sa_r.at[arr, h, s], z_to[0]).wait_send()
            for s in range(sb_n[arr]):
                ref = recv_b[arr].at[h, s]
                rcopy(ref, ref, sb_s.at[arr, h, s], sb_r.at[arr, h, s], z_to[0]).wait_send()
        ex_copy(arr, nx - 1).wait_send()


def solution(mesh):
    nz, ny, nd = mesh.shape["datb"], mesh.shape["model"], mesh.shape["data"]
    nx = nd // CORES

    def local_step(tok_loc, wg_loc, wu_loc, wd_loc, grad_loc):
        r, d_model = tok_loc.shape
        dp, fp = wg_loc.shape
        fo = fp // nd
        hf, zb, br = fo // 2, dp * nd, r * ny
        bh, rh = br // 2, r // 2
        vmem = pl.BlockSpec(memory_space=pltpu.VMEM)
        hbm = pl.BlockSpec(memory_space=pl.ANY)
        dma = pltpu.SemaphoreType.DMA
        most = max(nx, ny) - 1
        out, gin, dg, du, dd = pl.pallas_call(
            functools.partial(kernel, nz, ny, nx),
            out_shape=[jax.ShapeDtypeStruct((r, d_model), BF)] * 2 + [jax.ShapeDtypeStruct((dp, fp), F32)] * 3,
            in_specs=[hbm] * 5,
            out_specs=[vmem] * 5,
            scratch_shapes=[
                pltpu.VMEM((nx, CORES, br, d_model), BF),
                pltpu.VMEM((nx, CORES, br, d_model), BF),
                pltpu.VMEM((3, d_model, fo), BF),
                pltpu.VMEM((3, nd, br, fo), BF),
                pltpu.VMEM((3, fo, nd * br), BF),
                pltpu.VMEM((3, 2, 2, hf, zb), F32),
                pltpu.VMEM((3, 2, 2, hf, zb), F32),
                pltpu.VMEM((2, nx, br, d_model), BF),
                pltpu.VMEM((2, br, d_model), BF),
                pltpu.VMEM((2, nx - 1, bh, d_model), BF),
                pltpu.VMEM((2, ny - 1, nx, rh, d_model), BF),
                pltpu.VMEM((2, ny - 1, rh, d_model), BF),
                pltpu.VMEM((2, nx - 1, rh, d_model), BF),
                dma((5,)),
                dma((3, nd - 1)), dma((3, nd - 1)),
                dma((4, 2, nz - 1)), dma((4, 2, nz - 1)),
                dma((2, 2, most)), dma((2, 2, most)),
                dma((2, 2, most + 1, most)), dma((2, 2, most + 1, most)),
                dma((2, 2, most + 1, most + 1)), dma((2, 2, most + 1, most + 1)),
                dma((3, 2, nz - 1)), dma((3, 2, nz - 1)),
                pltpu.SemaphoreType.REGULAR((3, 2)),
                dma((2, nx)), dma((2, nx)),
                dma((2, 2, most)), dma((2, 2, most)),
                dma((2, 2, most)), dma((2, 2, most)),
                dma((3, 2, nd - 1)), dma((3, 2, nd - 1)),
            ],
            compiler_params=pltpu.CompilerParams(collective_id=0, has_side_effects=True, vmem_limit_bytes=67043328),
            name="swiglu_step",
        )(tok_loc, grad_loc, wg_loc, wu_loc, wd_loc.T)
        return out, gin, dg, du, dd.T

    return jax.shard_map(local_step, mesh=mesh, in_specs=(ROW_SPEC, GATE_SPEC, GATE_SPEC, DOWN_SPEC, ROW_SPEC), out_specs=(ROW_SPEC, ROW_SPEC, GATE_SPEC, GATE_SPEC, DOWN_SPEC), check_vma=False)
```

```python
import functools

import jax
import jax.numpy as jnp
from jax import lax
from jax.experimental import pallas as pl
from jax.experimental.pallas import tpu as pltpu
from jax.sharding import PartitionSpec as P

ROW_SPEC = P(("datb", "data", "model"), None)
GATE_SPEC = P(("datb", "data"), "model")
DOWN_SPEC = P("model", ("datb", "data"))
BF = jnp.bfloat16
F32 = jnp.float32
CORES = 2


def dot(lhs, rhs, ldim, rdim):
    return lax.dot_general(lhs, rhs, (((ldim,), (rdim,)), ((), ())), preferred_element_type=F32)


def sized(start, size):
    return pl.ds(pl.multiple_of(start, size), size)


def kernel(nz, ny, nx, tok_in, grad_in, wg_in, wu_in, wd_in, out_ref, gin_ref, dg_ref, du_ref, dd_ref,
           tok, grd, wgt, act, act_t, zrecv, zsend, ysum, stage, ya_recv, xa_recv, yb_recv, xb_recv,
           in_sem, a2a_s, a2a_r, ag_s, ag_r, p1_s, p1_r, p2_s, p2_r, pc_s, pc_r, rs_s, rs_r, credit,
           ex_s, ex_r, sa_s, sa_r, sb_s, sb_r, fa_s, fa_r, fo_sem):
    z, y, me = lax.axis_index("datb"), lax.axis_index("model"), lax.axis_index("data")
    x, c = me // CORES, lax.rem(me, CORES)
    nd = nx * CORES
    r, d_model = tok_in.shape
    dp, fp = wg_in.shape
    fo = fp // nd
    hf, zb, br = fo // 2, dp * nd, r * ny
    bh, rh = br // 2, r // 2

    z_to = ({"datb": lax.rem(z + 1, nz)}, {"datb": lax.rem(z + nz - 1, nz)})
    y_to = ({"model": lax.rem(y + 1, ny)}, {"model": lax.rem(y + ny - 1, ny)})
    x_to = ({"data": lax.rem(x + 1, nx) * CORES + c}, {"data": lax.rem(x + nx - 1, nx) * CORES + c})
    mate = {"data": x * CORES + 1 - c}

    def back(pos, n, d, s):
        return lax.rem(pos - s + 2 * n, n) if d == 0 else lax.rem(pos + s, n)

    def rcopy(src, dst, ss, rs, to):
        return pltpu.make_async_remote_copy(src_ref=src, dst_ref=dst, send_sem=ss, recv_sem=rs, device_id=to,
                                            device_id_type=pl.DeviceIdType.MESH)

    own = (tok.at[x, c, sized(y * r, r), :], grd.at[x, c, sized(y * r, r), :])
    w_in = (wg_in, wu_in, wd_in)
    moves = list(zip((tok_in, grad_in), own))
    moves += [(w_in[m].at[:, sized(me * fo, fo)], wgt.at[m, sized(z * zb + me * dp, dp), :]) for m in range(3)]
    loads = [pltpu.make_async_copy(src, dst, in_sem.at[i]) for i, (src, dst) in enumerate(moves)]
    for cp in loads:
        cp.start()
    barrier = pltpu.get_barrier_semaphore()
    peers = [{"data": lax.rem(me + k, nd)} for k in range(1, nd)]
    for to in peers + list(z_to) + list(y_to):
        pl.semaphore_signal(barrier, inc=1, device_id=to, device_id_type=pl.DeviceIdType.MESH)
    pl.semaphore_wait(barrier, nd - 1 + 4)

    def a2a(m, k):
        to = lax.rem(me + k, nd)
        return rcopy(w_in[m].at[:, sized(to * fo, fo)], wgt.at[m, sized(z * zb + me * dp, dp), :],
                     a2a_s.at[m, k - 1], a2a_r.at[m, k - 1], {"data": to})

    def a2a_wait(m, k):
        frm = lax.rem(me + nd - k, nd)
        dst = wgt.at[m, sized(z * zb + frm * dp, dp), :]
        rcopy(dst, dst, a2a_s.at[m, k - 1], a2a_r.at[m, k - 1], {"data": frm}).wait_recv()

    streams = ((0, 0, zb), (1, 0, zb), (2, 0, zb // 2), (2, zb // 2, zb // 2))

    def ag_copy(q, d, s, ahead):
        m, first, rows = streams[q]
        ref = wgt.at[m, sized(back(z, nz, d, s + ahead) * zb + first, rows), pl.ds(d * hf, hf)]
        return rcopy(ref, ref, ag_s.at[q, d, s], ag_r.at[q, d, s], z_to[d])

    def z_event(m, s):
        for q in range(4):
            if streams[q][0] == m:
                for d in (0, 1):
                    if s > 0:
                        ag_copy(q, d, s - 1, 1).wait_recv()
                    if s < nz - 1:
                        ag_copy(q, d, s, 0).start()

    first_n, second_n = (ny, nx), (nx, ny)
    first_to, second_to = (y_to, x_to), (x_to, y_to)

    def cell(arr, j, t, h, core):
        if arr == 0:
            return tok.at[back(x, nx, h, t), core, sized(back(y, ny, h, j) * r + h * rh, rh), :]
        return grd.at[back(x, nx, h, j), core, sized(back(y, ny, h, t) * r + h * rh, rh), :]

    def p1_copy(arr, h, j, ahead):
        ref = cell(arr, j + ahead, 0, h, c)
        return rcopy(ref, ref, p1_s.at[arr, h, j], p1_r.at[arr, h, j], first_to[arr][h])

    def p2_copy(arr, h, j, t, ahead):
        ref = cell(arr, j, t + ahead, h, c)
        return rcopy(ref, ref, p2_s.at[arr, h, j, t], p2_r.at[arr, h, j, t], second_to[arr][h])

    def pc_copy(arr, h, j, t, core):
        ref = cell(arr, j, t, h, core)
        return rcopy(ref, ref, pc_s.at[arr, h, j, t], pc_r.at[arr, h, j, t], mate)

    def token_event(j, t):
        for arr in (0, 1):
            if j < first_n[arr] and t < second_n[arr]:
                for h in (0, 1):
                    if t > 0:
                        p2_copy(arr, h, j, t - 1, 1).wait_recv()
                    elif j > 0:
                        p1_copy(arr, h, j - 1, 1).wait_recv()
                    if t == 0 and j < first_n[arr] - 1:
                        p1_copy(arr, h, j, 0).start()
                    if t < second_n[arr] - 1:
                        p2_copy(arr, h, j, t, 0).start()
                    pc_copy(arr, h, j, t, c).start()

    def a2a_event(m):
        for k in range(1, nd):
            a2a_wait(m, k)
        z_event(m, 0)

    for m in range(3):
        for k in range(1, nd):
            a2a(m, k).start()
    for cp in loads:
        cp.wait()

    most = max(nx, ny)
    marks = []
    sends = 0
    for ready, j, t in sorted((4.2 * j + 5.4 * t, j, t) for j in range(most) for t in range(most)):
        marks.append((10.0 * (j + t > 0) + max(ready, 3.4 * sends), len(marks), functools.partial(token_event, j, t)))
        sends += t < most - 1
    for m in range(3):
        marks.append((5.0 + 2.0 * m, len(marks), functools.partial(a2a_event, m)))
    ring_order = [(m, s) for s in range(1, nz) for m in (0, 1, 2)[: 3 if s % 2 == 0 else 2]]
    ring_order = [(m, s if m < 2 else s // 2) for m, s in ring_order]
    clock = 12.0
    for m, s in ring_order:
        marks.append((clock, len(marks), functools.partial(z_event, m, s)))
        clock += 2.8
    for _, _, f in sorted(marks, key=lambda mark: mark[:2]):
        f()
    late = [s for s in range(1, nz) if (2, s) not in ring_order]
    for arr in (0, 1):
        for h in (0, 1):
            for j in range(first_n[arr]):
                for t in range(second_n[arr]):
                    pc_copy(arr, h, j, t, 1 - c).wait_recv()

    def blocks(t):
        i, half = t // 2, lax.rem(t, 2)
        return i, i // CORES, lax.rem(i, CORES), sized(half * hf, hf)

    def forward_block(t, carry):
        i, xi, ci, sl = blocks(t)
        x_rows = tok[xi, ci]
        gate_b = dot(x_rows, wgt[0, :, sl], 1, 0).astype(BF)
        up_b = dot(x_rows, wgt[1, :, sl], 1, 0).astype(BF)
        gate_pre, up_pre = gate_b.astype(F32), up_b.astype(F32)
        hidden = (gate_pre * jax.nn.sigmoid(gate_pre) * up_pre).astype(BF)
        act[0, i, :, sl] = gate_b
        act[1, i, :, sl] = up_b
        act[2, i, :, sl] = hidden
        act_t[2, sl, sized(i * br, br)] = hidden.T
        for n, s in enumerate(late):

            @pl.when(t == (n + 1) * 2 * nd // len(late) - 1)
            def _():
                z_event(2, s)

        return carry

    lax.fori_loop(0, nd * 2, forward_block, 0)

    def backward_block(t, carry):
        i, xi, ci, sl = blocks(t)
        gate_pre, up_pre = act[0, i, :, sl].astype(F32), act[1, i, :, sl].astype(F32)
        grad_h = dot(grd[xi, ci], wgt[2, :, sl], 1, 0).astype(BF).astype(F32)
        sig = jax.nn.sigmoid(gate_pre)
        vals = ((grad_h * up_pre * sig * (1.0 + gate_pre * (1.0 - sig))).astype(BF), (grad_h * (gate_pre * sig)).astype(BF))
        for m in range(2):
            act[m, i, :, sl] = vals[m]
            act_t[m, sl, sized(i * br, br)] = vals[m].T
        return carry

    outs = (dg_ref, du_ref, dd_ref)

    def part(m, d, blk):
        src = grd if m == 2 else tok
        rhs = src[:, :, :, sized(blk * zb, zb)].reshape(nd * br, zb)
        return dot(act_t[m, pl.ds(d * hf, hf), :], rhs, 1, 0)

    def rs_copy(m, d, s):
        slot = lax.rem(s, 2)
        return rcopy(zsend.at[m, d, slot], zrecv.at[m, d, slot], rs_s.at[m, d, s], rs_r.at[m, d, s], z_to[d])

    def shift_of(d):
        return -1 if d == 0 else 1

    def rs_chunk(m, s, first):
        for d in (0, 1):
            blk = lax.rem(z - 1 - s + 2 * nz, nz) if d == 0 else lax.rem(z + 1 + s, nz)
            val = part(m, d, blk)
            if not first:
                rs_copy(m, d, s - 1).wait_recv()
                val = val + zrecv[m, d, lax.rem(s - 1, 2)]

                @pl.when(s >= 2)
                def _():
                    rs_copy(m, d, s - 2).wait_send()

            zsend[m, d, lax.rem(s, 2)] = val
            if not first:

                @pl.when(s <= nz - 3)
                def _():
                    pl.semaphore_signal(credit.at[m, d], inc=1, device_id=z_to[1 - d], device_id_type=pl.DeviceIdType.MESH)

                @pl.when(s >= 2)
                def _():
                    pl.semaphore_wait(credit.at[m, d], 1)

            rs_copy(m, d, s).start()

    order = (2, 0, 1)
    rs_chunk(2, 0, True)
    lax.fori_loop(0, nd, backward_block, 0)
    rs_chunk(2, 1, False)
    lax.fori_loop(nd, nd * 2, backward_block, 0)

    cols = d_model // 4

    def ex_copy(arr, xi):
        return rcopy(stage.at[arr], ysum.at[arr, xi], ex_s.at[arr, xi], ex_r.at[arr, xi], mate)

    def row_part(arr, i, j):
        sl = sized(j * cols, cols)
        if arr == 0:
            return dot(act[2, i], wgt[2, sl, :], 1, 1)
        return dot(act[0, i], wgt[0, sl, :], 1, 1) + dot(act[1, i], wgt[1, sl, :], 1, 1)

    def give(xi):
        for arr in (0, 1):
            if xi >= 1:
                ex_copy(arr, xi - 1).wait_send()

            def fill(j, carry):
                stage[arr, :, sized(j * cols, cols)] = row_part(arr, xi * CORES + 1 - c, j).astype(BF)
                return carry

            lax.fori_loop(0, d_model // cols, fill, 0)
            ex_copy(arr, xi).start()

    def keep(xi):
        for arr in (0, 1):
            ex_copy(arr, xi).wait_recv()

            def fill(j, carry):
                sl = sized(j * cols, cols)
                mine = row_part(arr, xi * CORES + c, j).astype(BF).astype(F32)
                ysum[arr, xi, :, sl] = (mine + ysum[arr, xi, :, sl].astype(F32)).astype(BF)
                return carry

            lax.fori_loop(0, d_model // cols, fill, 0)

    sa_n, sb_n = (nx - 1, ny - 1), (ny - 1, nx - 1)
    recv_a, recv_b = (ya_recv, xa_recv), (yb_recv, xb_recv)

    def sa_ref(arr, d, blk):
        if arr == 0:
            return ysum.at[0, blk, pl.ds(d * bh, bh), :]
        return ysum.at[1, :, sized(blk * r + d * rh, rh), :]

    def sb_ref(arr, d, blk):
        if arr == 0:
            return ysum.at[0, x, sized(blk * r + d * rh, rh), :]
        return ysum.at[1, blk, sized(y * r + d * rh, rh), :]

    def add_into(ref, slot):
        flat = len(ref.shape) == 2
        count = ref.shape[0] // 16 if flat else ref.shape[0]

        def piece(i, carry):
            at = sized(i * 16, 16) if flat else i
            ref[at] = (ref[at].astype(F32) + slot[at].astype(F32)).astype(BF)
            return carry

        lax.fori_loop(0, count, piece, 0)

    def scatter_event(refs, counts, recv, ss, rr, to, pos, s, last):
        for arr in (0, 1):
            n = counts[arr] + 1
            if s > counts[arr]:
                continue
            for d in (0, 1):
                blk = back(pos[arr] + shift_of(d), n, d, s)
                ref = refs(arr, d, blk)
                if s > 0:
                    slot = recv[arr].at[d, s - 1]
                    rcopy(slot, slot, ss.at[arr, d, s - 1], rr.at[arr, d, s - 1], to[arr][d]).wait_recv()
                    add_into(ref, slot)
                if s < counts[arr]:
                    rcopy(ref, recv[arr].at[d, s], ss.at[arr, d, s], rr.at[arr, d, s], to[arr][d]).start()

    def sa_event(s):
        scatter_event(sa_ref, sa_n, recv_a, sa_s, sa_r, (x_to, y_to), (x, y), s, False)

    def sb_event(s):
        scatter_event(sb_ref, sb_n, recv_b, sb_s, sb_r, (y_to, x_to), (y, x), s, True)

    def sb_finish():
        for arr, dst in ((0, out_ref), (1, gin_ref)):
            total = ysum[arr, x, sized(y * r, r), :].astype(F32)
            dst[...] = (own[arr][...].astype(F32) + total).astype(BF)

    spare = (nz - 1) % 2
    far = sorted(((g, e) for g in range(nx) for e in range(CORES) if g + e > 0), key=lambda ge: (-min(ge[0], nx - ge[0]), ge))

    def place(g, e):
        return lax.rem(x + g, nx) * CORES + (c if e == 0 else 1 - c)

    def fin_copy(m, d, g, e):
        to = place(g, e)
        return rcopy(zsend.at[m, d, spare, sized(to * dp, dp), :], outs[m].at[:, sized(me * fo + d * hf, hf)],
                     fa_s.at[m, d, g, e], fa_r.at[m, d, g, e], {"data": to})

    def fin_own(m, d):
        return pltpu.make_async_copy(zsend.at[m, d, spare, sized(me * dp, dp), :], outs[m].at[:, sized(me * fo + d * hf, hf)], fo_sem.at[m, d])

    def finish(m):
        for d in (0, 1):
            val = part(m, d, z)
            rs_copy(m, d, nz - 2).wait_recv()
            rs_copy(m, d, nz - 3).wait_send()
            zsend[m, d, spare] = (val + zrecv[m, d, nz % 2]).T
            for g, e in far:
                fin_copy(m, d, g, e).start()
            fin_own(m, d).start()

    slots = 3 * (nz - 1)
    work = [functools.partial(give, xi) for xi in range(nx)] + [functools.partial(keep, xi) for xi in range(nx)]
    plan = list(enumerate(work, 1))
    at = 1 + len(work)
    for s in range(max(sa_n) + 1):
        plan.append((at + 3 * s, functools.partial(sa_event, s)))
    at += 3 * max(sa_n)
    for s in range(max(sb_n) + 1):
        plan.append((at + s, functools.partial(sb_event, s)))
    plan.append((at + max(sb_n), sb_finish))

    for idx in (1, 2):
        rs_chunk(order[idx], 0, True)
        for slot, f in plan:
            if slot == idx:
                f()

    def ring(s, carry):
        for idx, m in enumerate(order):
            if m == 2:

                @pl.when(s <= nz - 3)
                def _():
                    rs_chunk(2, s + 1, False)

                @pl.when(s == nz - 2)
                def _():
                    finish(2)

            else:
                rs_chunk(m, s, False)
            for k in range(1, nz - 1):
                fs = [f for slot, f in plan if slot == 3 * k + idx]
                if fs:

                    @pl.when(s == k)
                    def _():
                        for f in fs:
                            f()

        return carry

    lax.fori_loop(1, nz - 1, ring, 0)
    for slot, f in plan:
        if slot >= slots:
            f()

    finish(0)
    finish(1)

    for m in order:
        for g, e in far:
            frm, back_g = place(g, e), (nx - g) % nx
            for d in (0, 1):
                dst = outs[m].at[:, sized(frm * fo + d * hf, hf)]
                rcopy(dst, dst, fa_s.at[m, d, back_g, e], fa_r.at[m, d, back_g, e], {"data": frm}).wait_recv()
                fin_copy(m, d, g, e).wait_send()
        for k in range(1, nd):
            a2a(m, k).wait_send()
        for d in (0, 1):
            fin_own(m, d).wait()
            rs_copy(m, d, nz - 2).wait_send()
    for q in range(4):
        for d in (0, 1):
            for s in range(nz - 1):
                ag_copy(q, d, s, 0).wait_send()
    for arr in (0, 1):
        for h in (0, 1):
            for j in range(first_n[arr]):
                if j < first_n[arr] - 1:
                    p1_copy(arr, h, j, 0).wait_send()
                for t in range(second_n[arr]):
                    if t < second_n[arr] - 1:
                        p2_copy(arr, h, j, t, 0).wait_send()
                    pc_copy(arr, h, j, t, c).wait_send()
            for s in range(sa_n[arr]):
                ref = recv_a[arr].at[h, s]
                rcopy(ref, ref, sa_s.at[arr, h, s], sa_r.at[arr, h, s], z_to[0]).wait_send()
            for s in range(sb_n[arr]):
                ref = recv_b[arr].at[h, s]
                rcopy(ref, ref, sb_s.at[arr, h, s], sb_r.at[arr, h, s], z_to[0]).wait_send()
        ex_copy(arr, nx - 1).wait_send()


def hand_on(*refs):
    for src, dst in zip(refs[:5], refs[5:]):
        dst[...] = src[...]


def solution(mesh):
    nz, ny, nd = mesh.shape["datb"], mesh.shape["model"], mesh.shape["data"]
    nx = nd // CORES

    def local_step(tok_loc, wg_loc, wu_loc, wd_loc, grad_loc):
        r, d_model = tok_loc.shape
        dp, fp = wg_loc.shape
        fo = fp // nd
        hf, zb, br = fo // 2, dp * nd, r * ny
        bh, rh = br // 2, r // 2
        vmem = pl.BlockSpec(memory_space=pltpu.VMEM)
        hbm = pl.BlockSpec(memory_space=pl.ANY)
        dma = pltpu.SemaphoreType.DMA
        most = max(nx, ny) - 1
        out, gin, dg, du, dd = pl.pallas_call(
            functools.partial(kernel, nz, ny, nx),
            out_shape=[jax.ShapeDtypeStruct((r, d_model), BF)] * 2 + [jax.ShapeDtypeStruct((dp, fp), F32)] * 3,
            in_specs=[hbm] * 5,
            out_specs=[vmem] * 2 + [hbm] * 3,
            scratch_shapes=[
                pltpu.VMEM((nx, CORES, br, d_model), BF),
                pltpu.VMEM((nx, CORES, br, d_model), BF),
                pltpu.VMEM((3, d_model, fo), BF),
                pltpu.VMEM((3, nd, br, fo), BF),
                pltpu.VMEM((3, fo, nd * br), BF),
                pltpu.VMEM((3, 2, 2, hf, zb), F32),
                pltpu.VMEM((3, 2, 2, hf, zb), F32),
                pltpu.VMEM((2, nx, br, d_model), BF),
                pltpu.VMEM((2, br, d_model), BF),
                pltpu.VMEM((2, nx - 1, bh, d_model), BF),
                pltpu.VMEM((2, ny - 1, nx, rh, d_model), BF),
                pltpu.VMEM((2, ny - 1, rh, d_model), BF),
                pltpu.VMEM((2, nx - 1, rh, d_model), BF),
                dma((5,)),
                dma((3, nd - 1)), dma((3, nd - 1)),
                dma((4, 2, nz - 1)), dma((4, 2, nz - 1)),
                dma((2, 2, most)), dma((2, 2, most)),
                dma((2, 2, most + 1, most)), dma((2, 2, most + 1, most)),
                dma((2, 2, most + 1, most + 1)), dma((2, 2, most + 1, most + 1)),
                dma((3, 2, nz - 1)), dma((3, 2, nz - 1)),
                pltpu.SemaphoreType.REGULAR((3, 2)),
                dma((2, nx)), dma((2, nx)),
                dma((2, 2, most)), dma((2, 2, most)),
                dma((2, 2, most)), dma((2, 2, most)),
                dma((3, 2, nx, CORES)), dma((3, 2, nx, CORES)), dma((3, 2)),
            ],
            compiler_params=pltpu.CompilerParams(collective_id=0, has_side_effects=True, vmem_limit_bytes=67043328),
            name="swiglu_step",
        )(tok_loc, grad_loc, wg_loc, wu_loc, wd_loc.T)
        out, gin, dg, du, dd = pl.pallas_call(
            hand_on,
            out_shape=[jax.ShapeDtypeStruct((r, d_model), BF)] * 2 + [jax.ShapeDtypeStruct((dp, fp), F32)] * 3,
            in_specs=[vmem] * 5,
            out_specs=[vmem] * 5,
            name="hand_on",
        )(out, gin, dg, du, dd)
        return out, gin, dg, du, dd.T

    return jax.shard_map(local_step, mesh=mesh, in_specs=(ROW_SPEC, GATE_SPEC, GATE_SPEC, DOWN_SPEC, ROW_SPEC), out_specs=(ROW_SPEC, ROW_SPEC, GATE_SPEC, GATE_SPEC, DOWN_SPEC), check_vma=False)
```

```python
import functools

import jax
import jax.numpy as jnp
from jax import lax
from jax.experimental import pallas as pl
from jax.experimental.pallas import tpu as pltpu
from jax.sharding import PartitionSpec as P

ROW_SPEC = P(("datb", "data", "model"), None)
GATE_SPEC = P(("datb", "data"), "model")
DOWN_SPEC = P("model", ("datb", "data"))
BF = jnp.bfloat16
F32 = jnp.float32
CORES = 2


def dot(lhs, rhs, ldim, rdim):
    return lax.dot_general(lhs, rhs, (((ldim,), (rdim,)), ((), ())), preferred_element_type=F32)


def sized(start, size):
    return pl.ds(pl.multiple_of(start, size), size)


def kernel(nz, ny, nx, tok_in, grad_in, wg_in, wu_in, wd_in, out_ref, gin_ref, dg_ref, du_ref, dd_ref,
           tok, grd, wgt, act, act_t, zrecv, zsend, ysum, stage, ya_recv, xa_recv, yb_recv, xb_recv,
           in_sem, a2a_s, a2a_r, ag_s, ag_r, p1_s, p1_r, p2_s, p2_r, pc_s, pc_r, rs_s, rs_r, credit,
           ex_s, ex_r, sa_s, sa_r, sb_s, sb_r, fa_s, fa_r, fo_sem):
    z, y, me = lax.axis_index("datb"), lax.axis_index("model"), lax.axis_index("data")
    x, c = me // CORES, lax.rem(me, CORES)
    nd = nx * CORES
    r, d_model = tok_in.shape
    dp, fp = wg_in.shape
    fo = fp // nd
    hf, zb, br = fo // 2, dp * nd, r * ny
    bh, rh = br // 2, r // 2

    z_to = ({"datb": lax.rem(z + 1, nz)}, {"datb": lax.rem(z + nz - 1, nz)})
    y_to = ({"model": lax.rem(y + 1, ny)}, {"model": lax.rem(y + ny - 1, ny)})
    x_to = ({"data": lax.rem(x + 1, nx) * CORES + c}, {"data": lax.rem(x + nx - 1, nx) * CORES + c})
    mate = {"data": x * CORES + 1 - c}

    def back(pos, n, d, s):
        return lax.rem(pos - s + 2 * n, n) if d == 0 else lax.rem(pos + s, n)

    def rcopy(src, dst, ss, rs, to):
        return pltpu.make_async_remote_copy(src_ref=src, dst_ref=dst, send_sem=ss, recv_sem=rs, device_id=to,
                                            device_id_type=pl.DeviceIdType.MESH)

    own = (tok.at[x, c, sized(y * r, r), :], grd.at[x, c, sized(y * r, r), :])
    w_in = (wg_in, wu_in, wd_in)
    moves = list(zip((tok_in, grad_in), own))
    moves += [(w_in[m].at[:, sized(me * fo, fo)], wgt.at[m, sized(z * zb + me * dp, dp), :]) for m in range(3)]
    loads = [pltpu.make_async_copy(src, dst, in_sem.at[i]) for i, (src, dst) in enumerate(moves)]
    for cp in loads:
        cp.start()
    barrier = pltpu.get_barrier_semaphore()
    peers = [{"data": lax.rem(me + k, nd)} for k in range(1, nd)]
    for to in peers + list(z_to) + list(y_to):
        pl.semaphore_signal(barrier, inc=1, device_id=to, device_id_type=pl.DeviceIdType.MESH)
    pl.semaphore_wait(barrier, nd - 1 + 4)

    def a2a(m, k):
        to = lax.rem(me + k, nd)
        return rcopy(w_in[m].at[:, sized(to * fo, fo)], wgt.at[m, sized(z * zb + me * dp, dp), :],
                     a2a_s.at[m, k - 1], a2a_r.at[m, k - 1], {"data": to})

    def a2a_wait(m, k):
        frm = lax.rem(me + nd - k, nd)
        dst = wgt.at[m, sized(z * zb + frm * dp, dp), :]
        rcopy(dst, dst, a2a_s.at[m, k - 1], a2a_r.at[m, k - 1], {"data": frm}).wait_recv()

    streams = ((0, 0, zb), (1, 0, zb), (2, 0, zb // 2), (2, zb // 2, zb // 2))

    def ag_copy(q, d, s, ahead):
        m, first, rows = streams[q]
        ref = wgt.at[m, sized(back(z, nz, d, s + ahead) * zb + first, rows), pl.ds(d * hf, hf)]
        return rcopy(ref, ref, ag_s.at[q, d, s], ag_r.at[q, d, s], z_to[d])

    def z_event(m, s):
        for q in range(4):
            if streams[q][0] == m:
                for d in (0, 1):
                    if s > 0:
                        ag_copy(q, d, s - 1, 1).wait_recv()
                    if s < nz - 1:
                        ag_copy(q, d, s, 0).start()

    first_n, second_n = (ny, nx), (nx, ny)
    first_to, second_to = (y_to, x_to), (x_to, y_to)

    def cell(arr, j, t, h, core):
        if arr == 0:
            return tok.at[back(x, nx, h, t), core, sized(back(y, ny, h, j) * r + h * rh, rh), :]
        return grd.at[back(x, nx, h, j), core, sized(back(y, ny, h, t) * r + h * rh, rh), :]

    def p1_copy(arr, h, j, ahead):
        ref = cell(arr, j + ahead, 0, h, c)
        return rcopy(ref, ref, p1_s.at[arr, h, j], p1_r.at[arr, h, j], first_to[arr][h])

    def p2_copy(arr, h, j, t, ahead):
        ref = cell(arr, j, t + ahead, h, c)
        return rcopy(ref, ref, p2_s.at[arr, h, j, t], p2_r.at[arr, h, j, t], second_to[arr][h])

    def pc_copy(arr, h, j, t, core):
        ref = cell(arr, j, t, h, core)
        return rcopy(ref, ref, pc_s.at[arr, h, j, t], pc_r.at[arr, h, j, t], mate)

    def token_event(j, t):
        for arr in (0, 1):
            if j < first_n[arr] and t < second_n[arr]:
                for h in (0, 1):
                    if t > 0:
                        p2_copy(arr, h, j, t - 1, 1).wait_recv()
                    elif j > 0:
                        p1_copy(arr, h, j - 1, 1).wait_recv()
                    if t == 0 and j < first_n[arr] - 1:
                        p1_copy(arr, h, j, 0).start()
                    if t < second_n[arr] - 1:
                        p2_copy(arr, h, j, t, 0).start()
                    pc_copy(arr, h, j, t, c).start()

    def a2a_event(m):
        for k in range(1, nd):
            a2a_wait(m, k)
        z_event(m, 0)

    for m in range(3):
        for k in range(1, nd):
            a2a(m, k).start()
    for cp in loads:
        cp.wait()

    most = max(nx, ny)
    marks = []
    sends = 0
    for ready, j, t in sorted((4.2 * j + 5.4 * t, j, t) for j in range(most) for t in range(most)):
        marks.append((10.0 * (j + t > 0) + max(ready, 3.4 * sends), len(marks), functools.partial(token_event, j, t)))
        sends += t < most - 1
    for m in range(3):
        marks.append((5.0 + 2.0 * m, len(marks), functools.partial(a2a_event, m)))
    ring_order = [(m, s) for s in range(1, nz) for m in (0, 1, 2)[: 3 if s % 2 == 0 else 2]]
    ring_order = [(m, s if m < 2 else s // 2) for m, s in ring_order]
    clock = 12.0
    for m, s in ring_order:
        marks.append((clock, len(marks), functools.partial(z_event, m, s)))
        clock += 2.8
    for _, _, f in sorted(marks, key=lambda mark: mark[:2]):
        f()
    late = [s for s in range(1, nz) if (2, s) not in ring_order]
    for arr in (0, 1):
        for h in (0, 1):
            for j in range(first_n[arr]):
                for t in range(second_n[arr]):
                    pc_copy(arr, h, j, t, 1 - c).wait_recv()

    def blocks(t):
        i, half = t // 2, lax.rem(t, 2)
        return i, i // CORES, lax.rem(i, CORES), sized(half * hf, hf)

    def forward_block(t, carry):
        i, xi, ci, sl = blocks(t)
        x_rows = tok[xi, ci]
        gate_b = dot(x_rows, wgt[0, :, sl], 1, 0).astype(BF)
        up_b = dot(x_rows, wgt[1, :, sl], 1, 0).astype(BF)
        gate_pre, up_pre = gate_b.astype(F32), up_b.astype(F32)
        hidden = (gate_pre * jax.nn.sigmoid(gate_pre) * up_pre).astype(BF)
        act[0, i, :, sl] = gate_b
        act[1, i, :, sl] = up_b
        act[2, i, :, sl] = hidden
        act_t[2, sl, sized(i * br, br)] = hidden.T
        for n, s in enumerate(late):

            @pl.when(t == (n + 1) * 2 * nd // len(late) - 1)
            def _():
                z_event(2, s)

        return carry

    lax.fori_loop(0, nd * 2, forward_block, 0)

    def backward_block(t, carry):
        i, xi, ci, sl = blocks(t)
        gate_pre, up_pre = act[0, i, :, sl].astype(F32), act[1, i, :, sl].astype(F32)
        grad_h = dot(grd[xi, ci], wgt[2, :, sl], 1, 0).astype(BF).astype(F32)
        sig = jax.nn.sigmoid(gate_pre)
        vals = ((grad_h * up_pre * sig * (1.0 + gate_pre * (1.0 - sig))).astype(BF), (grad_h * (gate_pre * sig)).astype(BF))
        for m in range(2):
            act[m, i, :, sl] = vals[m]
            act_t[m, sl, sized(i * br, br)] = vals[m].T
        return carry

    outs = (dg_ref, du_ref, dd_ref)

    def part(m, d, blk):
        src = grd if m == 2 else tok
        rhs = src[:, :, :, sized(blk * zb, zb)].reshape(nd * br, zb)
        return dot(act_t[m, pl.ds(d * hf, hf), :], rhs, 1, 0)

    def rs_copy(m, d, s):
        slot = lax.rem(s, 2)
        return rcopy(zsend.at[m, d, slot], zrecv.at[m, d, slot], rs_s.at[m, d, s], rs_r.at[m, d, s], z_to[d])

    def shift_of(d):
        return -1 if d == 0 else 1

    def rs_chunk(m, s, first):
        for d in (0, 1):
            blk = lax.rem(z - 1 - s + 2 * nz, nz) if d == 0 else lax.rem(z + 1 + s, nz)
            val = part(m, d, blk)
            if not first:
                rs_copy(m, d, s - 1).wait_recv()
                val = val + zrecv[m, d, lax.rem(s - 1, 2)]

                @pl.when(s >= 2)
                def _():
                    rs_copy(m, d, s - 2).wait_send()

            zsend[m, d, lax.rem(s, 2)] = val
            if not first:

                @pl.when(s <= nz - 3)
                def _():
                    pl.semaphore_signal(credit.at[m, d], inc=1, device_id=z_to[1 - d], device_id_type=pl.DeviceIdType.MESH)

                @pl.when(s >= 2)
                def _():
                    pl.semaphore_wait(credit.at[m, d], 1)

            rs_copy(m, d, s).start()

    order = (2, 0, 1)
    rs_chunk(2, 0, True)
    lax.fori_loop(0, nd * 2, backward_block, 0)

    cols = d_model // 4

    def ex_copy(arr, xi):
        return rcopy(stage.at[arr], ysum.at[arr, xi], ex_s.at[arr, xi], ex_r.at[arr, xi], mate)

    def row_part(arr, i, j):
        sl = sized(j * cols, cols)
        if arr == 0:
            return dot(act[2, i], wgt[2, sl, :], 1, 1)
        return dot(act[0, i], wgt[0, sl, :], 1, 1) + dot(act[1, i], wgt[1, sl, :], 1, 1)

    def give(xi):
        for arr in (0, 1):
            if xi >= 1:
                ex_copy(arr, xi - 1).wait_send()

            def fill(j, carry):
                stage[arr, :, sized(j * cols, cols)] = row_part(arr, xi * CORES + 1 - c, j).astype(BF)
                return carry

            lax.fori_loop(0, d_model // cols, fill, 0)
            ex_copy(arr, xi).start()

    def keep(xi):
        for arr in (0, 1):
            ex_copy(arr, xi).wait_recv()

            def fill(j, carry):
                sl = sized(j * cols, cols)
                mine = row_part(arr, xi * CORES + c, j).astype(BF).astype(F32)
                ysum[arr, xi, :, sl] = (mine + ysum[arr, xi, :, sl].astype(F32)).astype(BF)
                return carry

            lax.fori_loop(0, d_model // cols, fill, 0)

    sa_n, sb_n = (nx - 1, ny - 1), (ny - 1, nx - 1)
    recv_a, recv_b = (ya_recv, xa_recv), (yb_recv, xb_recv)

    def sa_ref(arr, d, blk):
        if arr == 0:
            return ysum.at[0, blk, pl.ds(d * bh, bh), :]
        return ysum.at[1, :, sized(blk * r + d * rh, rh), :]

    def sb_ref(arr, d, blk):
        if arr == 0:
            return ysum.at[0, x, sized(blk * r + d * rh, rh), :]
        return ysum.at[1, blk, sized(y * r + d * rh, rh), :]

    def add_into(ref, slot):
        flat = len(ref.shape) == 2
        count = ref.shape[0] // 16 if flat else ref.shape[0]

        def piece(i, carry):
            at = sized(i * 16, 16) if flat else i
            ref[at] = (ref[at].astype(F32) + slot[at].astype(F32)).astype(BF)
            return carry

        lax.fori_loop(0, count, piece, 0)

    def scatter_event(refs, counts, recv, ss, rr, to, pos, s, last):
        for arr in (0, 1):
            n = counts[arr] + 1
            if s > counts[arr]:
                continue
            for d in (0, 1):
                blk = back(pos[arr] + shift_of(d), n, d, s)
                ref = refs(arr, d, blk)
                if s > 0:
                    slot = recv[arr].at[d, s - 1]
                    rcopy(slot, slot, ss.at[arr, d, s - 1], rr.at[arr, d, s - 1], to[arr][d]).wait_recv()
                    add_into(ref, slot)
                if s < counts[arr]:
                    rcopy(ref, recv[arr].at[d, s], ss.at[arr, d, s], rr.at[arr, d, s], to[arr][d]).start()

    def sa_event(s):
        scatter_event(sa_ref, sa_n, recv_a, sa_s, sa_r, (x_to, y_to), (x, y), s, False)

    def sb_event(s):
        scatter_event(sb_ref, sb_n, recv_b, sb_s, sb_r, (y_to, x_to), (y, x), s, True)

    def sb_finish():
        for arr, dst in ((0, out_ref), (1, gin_ref)):
            total = ysum[arr, x, sized(y * r, r), :].astype(F32)
            dst[...] = (own[arr][...].astype(F32) + total).astype(BF)

    spare = (nz - 1) % 2
    far = sorted(((g, e) for g in range(nx) for e in range(CORES) if g + e > 0), key=lambda ge: (-min(ge[0], nx - ge[0]), ge))

    def place(g, e):
        return lax.rem(x + g, nx) * CORES + (c if e == 0 else 1 - c)

    def fin_copy(m, d, g, e):
        to = place(g, e)
        return rcopy(zsend.at[m, d, spare, sized(to * dp, dp), :], outs[m].at[:, sized(me * fo + d * hf, hf)],
                     fa_s.at[m, d, g, e], fa_r.at[m, d, g, e], {"data": to})

    def fin_own(m, d):
        return pltpu.make_async_copy(zsend.at[m, d, spare, sized(me * dp, dp), :], outs[m].at[:, sized(me * fo + d * hf, hf)], fo_sem.at[m, d])

    def finish(m):
        for d in (0, 1):
            val = part(m, d, z)
            rs_copy(m, d, nz - 2).wait_recv()
            rs_copy(m, d, nz - 3).wait_send()
            zsend[m, d, spare] = (val + zrecv[m, d, nz % 2]).T
            for g, e in far:
                fin_copy(m, d, g, e).start()
            fin_own(m, d).start()

    slots = 3 * (nz - 1)
    work = [functools.partial(give, xi) for xi in range(nx)] + [functools.partial(keep, xi) for xi in range(nx)]
    plan = list(enumerate(work, 1))
    at = 1 + len(work)
    for s in range(max(sa_n) + 1):
        plan.append((at + 8 * s // 3, functools.partial(sa_event, s)))
    at += 8 * max(sa_n) // 3
    for s in range(max(sb_n) + 1):
        plan.append((at + s, functools.partial(sb_event, s)))
    plan.append((at + max(sb_n), sb_finish))

    for idx in (1, 2):
        rs_chunk(order[idx], 0, True)
        if idx == 1:
            rs_chunk(2, 1, False)
        for slot, f in plan:
            if slot == idx:
                f()

    def ring(s, carry):
        for idx, m in enumerate(order):
            if m == 2:

                @pl.when(s <= nz - 3)
                def _():
                    rs_chunk(2, s + 1, False)

                @pl.when(s == nz - 2)
                def _():
                    finish(2)

            else:
                rs_chunk(m, s, False)
            for k in range(1, nz - 1):
                fs = [f for slot, f in plan if slot == 3 * k + idx]
                if fs:

                    @pl.when(s == k)
                    def _():
                        for f in fs:
                            f()

        return carry

    lax.fori_loop(1, nz - 1, ring, 0)
    for slot, f in plan:
        if slot >= slots:
            f()

    finish(0)
    finish(1)

    for m in order:
        for g, e in far:
            frm, back_g = place(g, e), (nx - g) % nx
            for d in (0, 1):
                dst = outs[m].at[:, sized(frm * fo + d * hf, hf)]
                rcopy(dst, dst, fa_s.at[m, d, back_g, e], fa_r.at[m, d, back_g, e], {"data": frm}).wait_recv()
                fin_copy(m, d, g, e).wait_send()
        for k in range(1, nd):
            a2a(m, k).wait_send()
        for d in (0, 1):
            fin_own(m, d).wait()
            rs_copy(m, d, nz - 2).wait_send()
    for q in range(4):
        for d in (0, 1):
            for s in range(nz - 1):
                ag_copy(q, d, s, 0).wait_send()
    for arr in (0, 1):
        for h in (0, 1):
            for j in range(first_n[arr]):
                if j < first_n[arr] - 1:
                    p1_copy(arr, h, j, 0).wait_send()
                for t in range(second_n[arr]):
                    if t < second_n[arr] - 1:
                        p2_copy(arr, h, j, t, 0).wait_send()
                    pc_copy(arr, h, j, t, c).wait_send()
            for s in range(sa_n[arr]):
                ref = recv_a[arr].at[h, s]
                rcopy(ref, ref, sa_s.at[arr, h, s], sa_r.at[arr, h, s], z_to[0]).wait_send()
            for s in range(sb_n[arr]):
                ref = recv_b[arr].at[h, s]
                rcopy(ref, ref, sb_s.at[arr, h, s], sb_r.at[arr, h, s], z_to[0]).wait_send()
        ex_copy(arr, nx - 1).wait_send()


def hand_on(*refs):
    for src, dst in zip(refs[:5], refs[5:]):
        dst[...] = src[...]


def solution(mesh):
    nz, ny, nd = mesh.shape["datb"], mesh.shape["model"], mesh.shape["data"]
    nx = nd // CORES

    def local_step(tok_loc, wg_loc, wu_loc, wd_loc, grad_loc):
        r, d_model = tok_loc.shape
        dp, fp = wg_loc.shape
        fo = fp // nd
        hf, zb, br = fo // 2, dp * nd, r * ny
        bh, rh = br // 2, r // 2
        vmem = pl.BlockSpec(memory_space=pltpu.VMEM)
        hbm = pl.BlockSpec(memory_space=pl.ANY)
        dma = pltpu.SemaphoreType.DMA
        most = max(nx, ny) - 1
        out, gin, dg, du, dd = pl.pallas_call(
            functools.partial(kernel, nz, ny, nx),
            out_shape=[jax.ShapeDtypeStruct((r, d_model), BF)] * 2 + [jax.ShapeDtypeStruct((dp, fp), F32)] * 3,
            in_specs=[hbm] * 5,
            out_specs=[vmem] * 2 + [hbm] * 3,
            scratch_shapes=[
                pltpu.VMEM((nx, CORES, br, d_model), BF),
                pltpu.VMEM((nx, CORES, br, d_model), BF),
                pltpu.VMEM((3, d_model, fo), BF),
                pltpu.VMEM((3, nd, br, fo), BF),
                pltpu.VMEM((3, fo, nd * br), BF),
                pltpu.VMEM((3, 2, 2, hf, zb), F32),
                pltpu.VMEM((3, 2, 2, hf, zb), F32),
                pltpu.VMEM((2, nx, br, d_model), BF),
                pltpu.VMEM((2, br, d_model), BF),
                pltpu.VMEM((2, nx - 1, bh, d_model), BF),
                pltpu.VMEM((2, ny - 1, nx, rh, d_model), BF),
                pltpu.VMEM((2, ny - 1, rh, d_model), BF),
                pltpu.VMEM((2, nx - 1, rh, d_model), BF),
                dma((5,)),
                dma((3, nd - 1)), dma((3, nd - 1)),
                dma((4, 2, nz - 1)), dma((4, 2, nz - 1)),
                dma((2, 2, most)), dma((2, 2, most)),
                dma((2, 2, most + 1, most)), dma((2, 2, most + 1, most)),
                dma((2, 2, most + 1, most + 1)), dma((2, 2, most + 1, most + 1)),
                dma((3, 2, nz - 1)), dma((3, 2, nz - 1)),
                pltpu.SemaphoreType.REGULAR((3, 2)),
                dma((2, nx)), dma((2, nx)),
                dma((2, 2, most)), dma((2, 2, most)),
                dma((2, 2, most)), dma((2, 2, most)),
                dma((3, 2, nx, CORES)), dma((3, 2, nx, CORES)), dma((3, 2)),
            ],
            compiler_params=pltpu.CompilerParams(collective_id=0, has_side_effects=True, vmem_limit_bytes=67043328),
            name="swiglu_step",
        )(tok_loc, grad_loc, wg_loc, wu_loc, wd_loc.T)
        out, gin, dg, du, dd = pl.pallas_call(
            hand_on,
            out_shape=[jax.ShapeDtypeStruct((r, d_model), BF)] * 2 + [jax.ShapeDtypeStruct((dp, fp), F32)] * 3,
            in_specs=[vmem] * 5,
            out_specs=[vmem] * 5,
            name="hand_on",
        )(out, gin, dg, du, dd)
        return out, gin, dg, du, dd.T

    return jax.shard_map(local_step, mesh=mesh, in_specs=(ROW_SPEC, GATE_SPEC, GATE_SPEC, DOWN_SPEC, ROW_SPEC), out_specs=(ROW_SPEC, ROW_SPEC, GATE_SPEC, GATE_SPEC, DOWN_SPEC), check_vma=False)
```
